512 devices in a mesh: layer: 4 (over x), row: 16 (over z, core), col: 8 (over y).
Axes of the slice: x: 4, y: 8, z: 8, core: 2. Of those that a mesh axis runs over, the one named last changes fastest.
Arguments:
- sources: bfloat16 [4, 96, 12288], P('layer', 'col', 'row'), may hold values from -6 to 6
- transmission: bfloat16 [4, 12288, 12288], P('layer', 'row', 'col'), may hold values from -0.0546875 to 0.0546875
- reflection: bfloat16 [4, 12288, 12288], P('layer', 'row', 'col'), may hold values from -0.02734375 to 0.02734375
Outputs:
- upgoing: bfloat16 [4, 96, 12288], P('layer', 'col', 'row')
The draws below stay inside these ranges and needn't reach their ends.
All inputs are finite; a program needn't handle non-finite values.
Results may differ from the reference program's by a relative error of at most 0.012.
Values may be sent and summed in bfloat16 or wider, within the bound.
No kernel may reach another device: no remote copies, remote signals or barrier semaphores. Data moves between devices by JAX's collectives and lax.ppermute only.
A program may use at most 64 MiB of HBM per device.

```python
import jax
import jax.numpy as jnp
from jax import lax

M = 12288
TRACES = 96
LAYERS = 4


def block_levels(own_key, dims, shards, smallest, high):
    gain, own = 1.0, jax.random.fold_in(own_key, 6)
    for position, shards_of in shards:
        steps = jnp.exp(jax.random.uniform(jax.random.fold_in(own, position), (shards_of,), jnp.float32, smallest / len(shards), high / len(shards)))
        gain = gain * jnp.repeat(steps, dims[position] // shards_of).reshape([-1 if axis == position else 1 for axis in range(len(dims))])
    return gain


def normal_values(rng, dims, spread, limit, shards=(), dtype=jnp.bfloat16):
    gain = block_levels(rng, dims, shards, -0.22, 0.18) if shards else 1.0
    entries = jax.random.normal(rng, dims, jnp.float32) * spread * gain
    return jnp.minimum(jnp.maximum(entries, -limit), limit).astype(dtype)


def setup_inputs(seed: int = 0) -> dict:
    key_of = jax.random.split(jax.random.key(seed), 4)
    sources = normal_values(key_of[0], (LAYERS, TRACES, M), 1.0, 6.0, ((0, 4), (1, 8), (2, 16)))
    transmission = normal_values(key_of[1], (LAYERS, M, M), M ** -0.5, 0.0546875, ((0, 4), (1, 16), (2, 8)))
    reflection = normal_values(key_of[2], (LAYERS, M, M), (4 * M) ** -0.5, 0.02734375, ((0, 4), (1, 16), (2, 8)))
    return {"sources": sources, "transmission": transmission, "reflection": reflection}


def reference(sources, transmission, reflection):
    down = jnp.zeros((TRACES, M), jnp.bfloat16)
    incidents = []
    for level in range(LAYERS):
        incident = (down.astype(jnp.float32) + sources[level].astype(jnp.float32)).astype(jnp.bfloat16)
        incidents.append(incident)
        down = jnp.dot(incident, transmission[level], preferred_element_type=jnp.float32).astype(jnp.bfloat16)
    upward = down
    results = [None] * LAYERS
    for level in reversed(range(LAYERS)):
        passed = lax.dot_general(upward, transmission[level], (((1,), (1,)), ((), ())), preferred_element_type=jnp.float32)
        bounced = lax.dot_general(incidents[level], reflection[level], (((1,), (1,)), ((), ())), preferred_element_type=jnp.float32)
        upward = (passed + bounced).astype(jnp.bfloat16)
        results[level] = upward
    return jnp.stack(results)
```

```python
import jax
import jax.numpy as jnp
import numpy as np
from jax import lax
from jax.sharding import Mesh, PartitionSpec as P

BF16 = jnp.bfloat16
F32 = jnp.float32
GRID = ("layer", "z", "core", "col")
ROW = ("z", "core")


def copy_for_each(array, axis):
    length = lax.axis_size(axis)
    return lax.all_to_all(
        jnp.broadcast_to(array[None], (length, *array.shape)), axis, 0, 0, tiled=True
    )


def summed_on_arrival(tiles, axis):
    arrived = lax.all_to_all(tiles, axis, split_axis=0, concat_axis=0, tiled=True)
    return arrived.astype(F32).sum(axis=0).astype(BF16)


def per_device(sources, transmission, reflection):
    layers = lax.axis_size("layer")
    zs = lax.axis_size("z")
    cores = lax.axis_size("core")
    cols = lax.axis_size("col")
    half = zs // 2
    layer_index = lax.axis_index("layer")
    col_index = lax.axis_index("col")
    trans_tile = transmission[0]
    reflect_tile = reflection[0]
    row_width, col_width = trans_tile.shape
    few = sources.shape[1]
    traces = few * cols
    group, part = 2 * few, row_width // 2

    def flat(l, z, k, y):
        return ((l * zs + z) * cores + k) * cols + y

    def cells(layer_range):
        for l in layer_range:
            for z in range(zs):
                for k in range(cores):
                    for y in range(cols):
                        yield l, z, k, y

    down_pairs = [
        (flat(l, z, k, y), flat(l + 1, y, k, (z + half) % zs))
        for l, z, k, y in cells(range(layers - 1))
    ]
    back_pairs = [
        (flat(l, y, k, (z + half) % zs), flat(l, z, k, y)) for l, z, k, y in cells(range(layers))
    ]
    up_pairs = [
        (flat(l, z, k, y), flat(l - 1, (y + half) % zs, k, z))
        for l, z, k, y in cells(range(1, layers))
    ]

    def whole_block(pieces):
        tiles = pieces.reshape(cols // 2, 2, group, part)
        return tiles.transpose(0, 2, 1, 3).reshape(traces, row_width)

    source_narrow = copy_for_each(sources[0], "col").reshape(traces, row_width)
    incident = source_narrow
    share = None
    incident_share = None
    for step in range(layers):
        if step > 0:
            moved = lax.ppermute(share, GRID, down_pairs)
            incoming = whole_block(copy_for_each(moved, "col"))
            incident = (incoming.astype(F32) + source_narrow.astype(F32)).astype(BF16)
        if step == layers - 1:
            own = incident.reshape(cols // 2, group, 2, part).transpose(0, 2, 1, 3)
            own = own.reshape(cols, group, part)
            own = lax.dynamic_index_in_dim(own, col_index, 0, keepdims=False)
            incident_share = lax.ppermute(own, GRID, back_pairs)
        partial = jnp.dot(incident, trans_tile, preferred_element_type=F32).astype(BF16)
        tiles = partial.reshape(cols // 2, group, cores, 2, part).transpose(0, 3, 2, 1, 4)
        tiles = jnp.roll(tiles.reshape(zs, cores, group, part), -half, axis=0)
        share = summed_on_arrival(tiles.reshape(zs * cores, group, part), ROW)

    both = copy_for_each(jnp.stack([share, incident_share]), "z")
    both = jnp.roll(both, half, axis=0)
    both = lax.all_gather(both, "core")
    both = both.reshape(cores, cols // 2, 2, 2, group, part).transpose(3, 1, 4, 0, 2, 5)
    both = both.reshape(2, traces, col_width)
    contract = (((1,), (1,)), ((), ()))
    bounced = lax.dot_general(both[1], reflect_tile, contract, preferred_element_type=F32)
    upward = both[0]
    result = jnp.zeros((few, row_width), BF16)
    for step in range(layers):
        if step > 0:
            moved = lax.ppermute(newest, GRID, up_pairs)
            wide = jnp.roll(copy_for_each(moved, "z"), half, axis=0)
            wide = lax.all_gather(wide.reshape(traces, row_width), "core")
            upward = wide.transpose(1, 0, 2).reshape(traces, col_width)
        passed = lax.dot_general(upward, trans_tile, contract, preferred_element_type=F32)
        partial = (passed + bounced).astype(BF16)
        newest = summed_on_arrival(partial.reshape(cols, few, row_width), "col")
        result = jnp.where(layer_index == layers - 1 - step, newest, result)
    return result[None]


def solution(mesh):
    layers, rows, cols = mesh.devices.shape
    grid = Mesh(np.array(mesh.devices).reshape(layers, rows // 2, 2, cols), GRID)
    return jax.shard_map(
        per_device,
        mesh=grid,
        in_specs=(P("layer", "col", ROW), P("layer", ROW, "col"), P("layer", ROW, "col")),
        out_specs=P("layer", "col", ROW),
        check_vma=False,
    )
```

```python
import jax
import jax.numpy as jnp
import numpy as np
from jax import lax
from jax.sharding import Mesh, PartitionSpec as P

BF16 = jnp.bfloat16
F32 = jnp.float32
GRID = ("layer", "z", "core", "col")
ROW = ("z", "core")


def copy_for_each(array, axis):
    length = lax.axis_size(axis)
    return lax.all_to_all(
        jnp.broadcast_to(array[None], (length, *array.shape)), axis, 0, 0, tiled=True
    )


def summed_on_arrival(tiles, axis):
    arrived = lax.all_to_all(tiles, axis, split_axis=0, concat_axis=0, tiled=True)
    return arrived.astype(F32).sum(axis=0).astype(BF16)


def added(a, b):
    return (a.astype(F32) + b.astype(F32)).astype(BF16)


def per_device(sources, transmission, reflection):
    layers = lax.axis_size("layer")
    zs = lax.axis_size("z")
    cores = lax.axis_size("core")
    cols = lax.axis_size("col")
    half = zs // 2
    layer_index = lax.axis_index("layer")
    col_index = lax.axis_index("col")
    trans_tile = transmission[0]
    reflect_tile = reflection[0]
    row_width, col_width = trans_tile.shape
    few = sources.shape[1]
    traces = few * cols
    group, part = 2 * few, row_width // 2

    def flat(l, z, k, y):
        return ((l * zs + z) * cores + k) * cols + y

    def cells(layer_range):
        for l in layer_range:
            for z in range(zs):
                for k in range(cores):
                    for y in range(cols):
                        yield l, z, k, y

    down_pairs = [
        (flat(l, z, k, y), flat(l + 1, y, k, (z + half) % zs))
        for l, z, k, y in cells(range(layers - 1))
    ]
    back_pairs = [
        (flat(l, y, k, (z + half) % zs), flat(l, z, k, y)) for l, z, k, y in cells(range(layers))
    ]
    below_pairs = [
        (flat(l, z, k, y), flat(l + 1, z, k, y)) for l, z, k, y in cells(range(layers - 1))
    ]
    up_pairs = [
        (flat(l, z, k, y), flat(l - 1, (y + half) % zs, k, z))
        for l, z, k, y in cells(range(1, layers))
    ]

    def whole_block(pieces):
        tiles = pieces.reshape(cols // 2, 2, group, part)
        return tiles.transpose(0, 2, 1, 3).reshape(traces, row_width)

    def share_of_down(incident):
        partial = jnp.dot(incident, trans_tile, preferred_element_type=F32).astype(BF16)
        tiles = partial.reshape(cols // 2, group, cores, 2, part).transpose(0, 3, 2, 1, 4)
        tiles = jnp.roll(tiles.reshape(zs, cores, group, part), -half, axis=0)
        return summed_on_arrival(tiles.reshape(zs * cores, group, part), ROW)

    def nothing(array, shape=(group, part)):
        return jnp.zeros(shape, BF16)

    source_narrow = copy_for_each(sources[0], "col").reshape(traces, row_width)

    def on_arrival(moved):
        return share_of_down(added(whole_block(copy_for_each(moved, "col")), source_narrow))

    share = lax.cond(layer_index == 0, share_of_down, nothing, source_narrow)
    own = source_narrow.reshape(cols // 2, group, 2, part).transpose(0, 2, 1, 3)
    own = lax.dynamic_index_in_dim(own.reshape(cols, group, part), col_index, 0, keepdims=False)
    source_share = None
    above = jnp.zeros((group, part), BF16)
    for step in range(1, layers):
        moved = lax.ppermute(share, GRID, down_pairs)
        if step == 1:
            source_share = lax.ppermute(own, GRID, back_pairs)
        above = jnp.where(layer_index == step, lax.ppermute(share, GRID, below_pairs), above)
        share = lax.cond(layer_index == step, on_arrival, nothing, moved)

    both = copy_for_each(jnp.stack([share, added(above, source_share)]), "z")
    both = jnp.roll(both, half, axis=0)
    both = lax.all_gather(both, "core")
    both = both.reshape(cores, cols // 2, 2, 2, group, part).transpose(3, 1, 4, 0, 2, 5)
    both = both.reshape(2, traces, col_width)
    contract = (((1,), (1,)), ((), ()))
    bounced = lax.dot_general(both[1], reflect_tile, contract, preferred_element_type=F32)

    def share_of_up(upward):
        passed = lax.dot_general(upward, trans_tile, contract, preferred_element_type=F32)
        partial = (passed + bounced).astype(BF16)
        return summed_on_arrival(partial.reshape(cols, few, row_width), "col")

    def on_return(moved):
        wide = jnp.roll(copy_for_each(moved, "z"), half, axis=0)
        wide = lax.all_gather(wide.reshape(traces, row_width), "core")
        return share_of_up(wide.transpose(1, 0, 2).reshape(traces, col_width))

    def nothing_up(array):
        return nothing(array, (few, row_width))

    result = newest = share_of_up(both[0])
    for step in range(1, layers):
        moved = lax.ppermute(newest, GRID, up_pairs)
        turn = layer_index == layers - 1 - step
        newest = lax.cond(turn, on_return, nothing_up, moved)
        result = jnp.where(turn, newest, result)
    return result[None]


def solution(mesh):
    layers, rows, cols = mesh.devices.shape
    grid = Mesh(np.array(mesh.devices).reshape(layers, rows // 2, 2, cols), GRID)
    return jax.shard_map(
        per_device,
        mesh=grid,
        in_specs=(P("layer", "col", ROW), P("layer", ROW, "col"), P("layer", ROW, "col")),
        out_specs=P("layer", "col", ROW),
        check_vma=False,
    )
```

```python
import jax
import jax.numpy as jnp
import numpy as np
from jax import lax
from jax.sharding import Mesh, PartitionSpec as P

BF16 = jnp.bfloat16
F32 = jnp.float32
GRID = ("layer", "z", "core", "col")
ROW = ("z", "core")


def copy_for_each(array, axis):
    length = lax.axis_size(axis)
    return lax.all_to_all(
        jnp.broadcast_to(array[None], (length, *array.shape)), axis, 0, 0, tiled=True
    )


def summed_on_arrival(tiles, axis):
    arrived = lax.all_to_all(tiles, axis, split_axis=0, concat_axis=0, tiled=True)
    return arrived.astype(F32).sum(axis=0).astype(BF16)


def added(a, b):
    return (a.astype(F32) + b.astype(F32)).astype(BF16)


def per_device(sources, transmission, reflection):
    layers = lax.axis_size("layer")
    zs = lax.axis_size("z")
    cores = lax.axis_size("core")
    cols = lax.axis_size("col")
    half = zs // 2
    layer_index = lax.axis_index("layer")
    col_index = lax.axis_index("col")
    trans_tile = transmission[0]
    reflect_tile = reflection[0]
    row_width, col_width = trans_tile.shape
    few = sources.shape[1]
    traces = few * cols
    group, part = 2 * few, row_width // 2

    def flat(l, z, k, y):
        return ((l * zs + z) * cores + k) * cols + y

    def cells(layer_range):
        for l in layer_range:
            for z in range(zs):
                for k in range(cores):
                    for y in range(cols):
                        yield l, z, k, y

    far_first = [half] + [d for k in range(1, half) for d in (half - k, half + k)] + [0]

    def down_pairs(d):
        return [
            (flat(l, z, k, y), flat(l + 1, y, k, (z + half + d) % zs))
            for l, z, k, y in cells(range(layers - 1))
        ]

    def up_pairs(d):
        return [
            (flat(l, z, k, y), flat(l - 1, (y + half + d) % zs, k, z))
            for l, z, k, y in cells(range(1, layers))
        ]

    back_pairs = [
        (flat(l, y, k, z), flat(l, z, k, y)) for l, z, k, y in cells(range(layers))
    ]
    below_pairs = [
        (flat(l, z, k, y), flat(l + 1, z, k, y)) for l, z, k, y in cells(range(layers - 1))
    ]

    def spread(share, pairs, place):
        arrived = [(d, lax.ppermute(share, GRID, pairs(d))) for d in far_first]
        pieces = jnp.zeros((cols, *share.shape), BF16)
        for d, piece in arrived:
            pieces = lax.dynamic_update_index_in_dim(pieces, piece, (place - half - d) % cols, 0)
        return pieces

    def whole_block(pieces):
        tiles = pieces.reshape(cols // 2, 2, group, part)
        return tiles.transpose(0, 2, 1, 3).reshape(traces, row_width)

    def down_tiles(incident):
        partial = jnp.dot(incident, trans_tile, preferred_element_type=F32).astype(BF16)
        tiles = partial.reshape(cols // 2, group, cores, 2, part).transpose(0, 3, 2, 1, 4)
        return tiles.reshape(zs * cores, group, part)

    def reduced(turn, tiles, axis):
        return lax.cond(
            turn,
            lambda t: summed_on_arrival(t, axis),
            lambda t: jnp.zeros(t.shape[1:], BF16),
            tiles,
        )

    source_narrow = copy_for_each(sources[0], "col").reshape(traces, row_width)
    own = source_narrow.reshape(cols // 2, group, 2, part).transpose(0, 2, 1, 3)
    own = lax.dynamic_index_in_dim(own.reshape(cols, group, part), col_index, 0, keepdims=False)
    share = reduced(layer_index == 0, down_tiles(source_narrow), ROW)
    sent = share
    for step in range(1, layers):
        pieces = spread(share, down_pairs, col_index)
        if step == 1:
            source_share = lax.ppermute(own, GRID, back_pairs)
            pieces, source_share = lax.optimization_barrier((pieces, source_share))
        if step == layers - 1:
            above = lax.ppermute(sent, GRID, below_pairs)
        turn = layer_index == step
        share = reduced(turn, down_tiles(added(whole_block(pieces), source_narrow)), ROW)
        sent = jnp.where(turn, share, sent)

    both = copy_for_each(jnp.stack([share, added(above, source_share)]), "z")
    both = lax.all_gather(both, "core")
    both = both.reshape(cores, cols // 2, 2, 2, group, part).transpose(3, 1, 4, 0, 2, 5)
    both = both.reshape(2, traces, col_width)
    contract = (((1,), (1,)), ((), ()))
    bounced = lax.dot_general(both[1], reflect_tile, contract, preferred_element_type=F32)

    def up_tiles(upward):
        passed = lax.dot_general(upward, trans_tile, contract, preferred_element_type=F32)
        return (passed + bounced).astype(BF16).reshape(cols, few, row_width)

    result = newest = reduced(layer_index == layers - 1, up_tiles(both[0]), "col")
    for step in range(1, layers):
        wide = spread(newest, up_pairs, lax.axis_index("z"))
        wide = lax.all_gather(wide.reshape(traces, row_width), "core")
        upward = wide.transpose(1, 0, 2).reshape(traces, col_width)
        turn = layer_index == layers - 1 - step
        newest = reduced(turn, up_tiles(upward), "col")
        result = jnp.where(turn, newest, result)
    return result[None]


def solution(mesh):
    layers, rows, cols = mesh.devices.shape
    grid = Mesh(np.array(mesh.devices).reshape(layers, rows // 2, 2, cols), GRID)
    return jax.shard_map(
        per_device,
        mesh=grid,
        in_specs=(P("layer", "col", ROW), P("layer", ROW, "col"), P("layer", ROW, "col")),
        out_specs=P("layer", "col", ROW),
        check_vma=False,
    )
```

```python
import jax
import jax.numpy as jnp
import numpy as np
from jax import lax
from jax.sharding import Mesh, PartitionSpec as P

BF16 = jnp.bfloat16
F32 = jnp.float32
GRID = ("layer", "z", "core", "col")
ROW = ("z", "core")


def copy_for_each(array, axis):
    length = lax.axis_size(axis)
    return lax.all_to_all(
        jnp.broadcast_to(array[None], (length, *array.shape)), axis, 0, 0, tiled=True
    )


def summed_on_arrival(tiles, axis):
    arrived = lax.all_to_all(tiles, axis, split_axis=0, concat_axis=0, tiled=True)
    return arrived.astype(F32).sum(axis=0).astype(BF16)


def added(a, b):
    return (a.astype(F32) + b.astype(F32)).astype(BF16)


def per_device(sources, transmission, reflection):
    layers = lax.axis_size("layer")
    zs = lax.axis_size("z")
    cores = lax.axis_size("core")
    cols = lax.axis_size("col")
    half = zs // 2
    layer_index = lax.axis_index("layer")
    col_index = lax.axis_index("col")
    trans_tile = transmission[0]
    reflect_tile = reflection[0]
    row_width, col_width = trans_tile.shape
    few = sources.shape[1]
    traces = few * cols
    group, part = 2 * few, row_width // 2

    def flat(l, z, k, y):
        return ((l * zs + z) * cores + k) * cols + y

    def cells(layer_range):
        for l in layer_range:
            for z in range(zs):
                for k in range(cores):
                    for y in range(cols):
                        yield l, z, k, y

    far_first = [half, half // 2, zs - half // 2, 0]
    neighbours = [[i, i + 1] for i in range(0, cols, 2)]

    def down_pairs(d):
        return [
            (flat(l, z, k, y), flat(l + 1, y, k, (z + half + d) % zs))
            for l, z, k, y in cells(range(layers - 1))
        ]

    def up_pairs(d):
        return [
            (flat(l, z, k, y), flat(l - 1, (y + half + d) % zs, k, z))
            for l, z, k, y in cells(range(1, layers))
        ]

    back_pairs = [
        (flat(l, y, k, z), flat(l, z, k, y)) for l, z, k, y in cells(range(layers))
    ]
    below_pairs = [
        (flat(l, z, k, y), flat(l + 1, z, k, y)) for l, z, k, y in cells(range(layers - 1))
    ]

    def spread(share, pairs, axis):
        arrived = [(d, lax.ppermute(share, GRID, pairs(d))) for d in far_first]
        pieces = jnp.zeros((half, *share.shape), BF16)
        for d, piece in arrived:
            place = (lax.axis_index(axis) - half - d) % zs // 2
            pieces = lax.dynamic_update_index_in_dim(pieces, piece, place, 0)
        return lax.all_gather(pieces, axis, axis_index_groups=neighbours)

    def whole_block(pieces):
        return pieces.transpose(1, 2, 0, 3).reshape(traces, row_width)

    def down_tiles(incident):
        partial = jnp.dot(incident, trans_tile, preferred_element_type=F32).astype(BF16)
        tiles = partial.reshape(cols // 2, group, cores, 2, part).transpose(0, 3, 2, 1, 4)
        return tiles.reshape(zs * cores, group, part)

    def reduced(turn, tiles, axis):
        return lax.cond(
            turn,
            lambda t: summed_on_arrival(t, axis),
            lambda t: jnp.zeros(t.shape[1:], BF16),
            tiles,
        )

    source_narrow = copy_for_each(sources[0], "col").reshape(traces, row_width)
    own = source_narrow.reshape(cols // 2, group, 2, part).transpose(0, 2, 1, 3)
    own = lax.dynamic_index_in_dim(own.reshape(cols, group, part), col_index, 0, keepdims=False)
    share = reduced(layer_index == 0, down_tiles(source_narrow), ROW)
    sent = share
    for step in range(1, layers):
        pieces = spread(share, down_pairs, "col")
        if step == 1:
            source_share = lax.ppermute(own, GRID, back_pairs)
            pieces, source_share = lax.optimization_barrier((pieces, source_share))
        if step == layers - 1:
            above = lax.ppermute(sent, GRID, below_pairs)
        turn = layer_index == step
        share = reduced(turn, down_tiles(added(whole_block(pieces), source_narrow)), ROW)
        sent = jnp.where(turn, share, sent)

    both = copy_for_each(jnp.stack([share, added(above, source_share)]), "z")
    both = lax.all_gather(both, "core")
    both = both.reshape(cores, cols // 2, 2, 2, group, part).transpose(3, 1, 4, 0, 2, 5)
    both = both.reshape(2, traces, col_width)
    contract = (((1,), (1,)), ((), ()))
    bounced = lax.dot_general(both[1], reflect_tile, contract, preferred_element_type=F32)

    bounced = bounced.reshape(cols, few, row_width)

    def times_trans(rows):
        return lax.dot_general(rows, trans_tile, contract, preferred_element_type=F32)

    room = -few % 16

    def padded(share):
        return jnp.concatenate([share, share[few - room :]])

    def share_of_up(turn, passed):
        return lax.cond(
            turn,
            lambda p, b: padded(summed_on_arrival((p + b).astype(BF16), "col")),
            lambda p, b: jnp.zeros((few + room, row_width), BF16),
            passed,
            bounced,
        )

    passed = times_trans(both[0]).reshape(cols, few, row_width)
    result = newest = share_of_up(layer_index == layers - 1, passed)
    for step in range(1, layers):
        pieces = spread(newest, up_pairs, "z")
        wide = lax.all_gather(pieces, "core").reshape(cores, -1, row_width)
        passed = times_trans(wide.transpose(1, 0, 2).reshape(-1, col_width))
        passed = passed.reshape(2, half, few + room, row_width)[:, :, :few]
        passed = passed.transpose(1, 0, 2, 3).reshape(cols, few, row_width)
        turn = layer_index == layers - 1 - step
        newest = share_of_up(turn, passed)
        result = jnp.where(turn, newest, result)
    return result[None, :few]


def solution(mesh):
    layers, rows, cols = mesh.devices.shape
    grid = Mesh(np.array(mesh.devices).reshape(layers, rows // 2, 2, cols), GRID)
    return jax.shard_map(
        per_device,
        mesh=grid,
        in_specs=(P("layer", "col", ROW), P("layer", ROW, "col"), P("layer", ROW, "col")),
        out_specs=P("layer", "col", ROW),
        check_vma=False,
    )
```

```python
import jax
import jax.numpy as jnp
import numpy as np
from jax import lax
from jax.sharding import Mesh, PartitionSpec as P

BF16 = jnp.bfloat16
F32 = jnp.float32
GRID = ("layer", "z", "core", "col")
ROW = ("z", "core")


def copy_for_each(array, axis):
    length = lax.axis_size(axis)
    return lax.all_to_all(
        jnp.broadcast_to(array[None], (length, *array.shape)), axis, 0, 0, tiled=True
    )


def summed_on_arrival(tiles, axis):
    arrived = lax.all_to_all(tiles, axis, split_axis=0, concat_axis=0, tiled=True)
    return arrived.astype(F32).sum(axis=0).astype(BF16)


def added(a, b):
    return (a.astype(F32) + b.astype(F32)).astype(BF16)


def per_device(sources, transmission, reflection):
    layers = lax.axis_size("layer")
    zs = lax.axis_size("z")
    cores = lax.axis_size("core")
    cols = lax.axis_size("col")
    half = zs // 2
    layer_index = lax.axis_index("layer")
    col_index = lax.axis_index("col")
    trans_tile = transmission[0]
    reflect_tile = reflection[0]
    row_width, col_width = trans_tile.shape
    few = sources.shape[1]
    traces = few * cols
    group, part = 2 * few, row_width // 2

    def flat(l, z, k, y):
        return ((l * zs + z) * cores + k) * cols + y

    def cells(layer_range):
        for l in layer_range:
            for z in range(zs):
                for k in range(cores):
                    for y in range(cols):
                        yield l, z, k, y

    far_first = [half, half // 2, zs - half // 2, 0]
    neighbours = [[i, i + 1] for i in range(0, cols, 2)]

    def down_pairs(d):
        return [
            (flat(l, z, k, y), flat(l + 1, y, k, (z + half + d) % zs))
            for l, z, k, y in cells(range(layers - 1))
        ]

    def up_pairs(d):
        return [
            (flat(l, z, k, y), flat(l - 1, (y + half + d) % zs, k, z))
            for l, z, k, y in cells(range(1, layers))
        ]

    back_pairs = [
        (flat(l, y, k, z), flat(l, z, k, y)) for l, z, k, y in cells(range(layers))
    ]
    below_pairs = [
        (flat(l, z, k, y), flat(l + 1, z, k, y)) for l, z, k, y in cells(range(layers - 1))
    ]

    def spread(share, pairs, axis):
        arrived = [(d, lax.ppermute(share, GRID, pairs(d))) for d in far_first]
        pieces = jnp.zeros((half, *share.shape), BF16)
        for d, piece in arrived:
            place = (lax.axis_index(axis) - half - d) % zs // 2
            pieces = lax.dynamic_update_index_in_dim(pieces, piece, place, 0)
        return lax.all_gather(pieces, axis, axis_index_groups=neighbours)

    def whole_block(pieces):
        return pieces.transpose(1, 2, 0, 3).reshape(traces, row_width)

    def down_tiles(incident):
        partial = jnp.dot(incident, trans_tile, preferred_element_type=F32).astype(BF16)
        tiles = partial.reshape(cols // 2, group, cores, 2, part).transpose(0, 3, 2, 1, 4)
        return tiles.reshape(zs * cores, group, part)

    def reduced(turn, tiles, axis):
        return lax.cond(
            turn,
            lambda t: summed_on_arrival(t, axis),
            lambda t: jnp.zeros(t.shape[1:], BF16),
            tiles,
        )

    always = layer_index < layers

    def copied(array, axis, shape):
        return lax.cond(
            always,
            lambda a: copy_for_each(a, axis).reshape(shape),
            lambda a: jnp.zeros(shape, BF16),
            array,
        )

    source_narrow = copied(sources[0], "col", (traces, row_width))
    source_narrow = lax.optimization_barrier(source_narrow)
    own = source_narrow.reshape(cols // 2, group, 2, part).transpose(0, 2, 1, 3)
    own = lax.dynamic_index_in_dim(own.reshape(cols, group, part), col_index, 0, keepdims=False)
    share = reduced(layer_index == 0, down_tiles(source_narrow), ROW)
    sent = share
    for step in range(1, layers):
        pieces = spread(share, down_pairs, "col")
        if step == 1:
            source_share = lax.ppermute(own, GRID, back_pairs)
            near_tile = jnp.where(always, reflect_tile, jnp.zeros((), BF16))
            pieces, source_share, near_tile = lax.optimization_barrier(
                (pieces, source_share, near_tile)
            )
        if step == layers - 1:
            above = lax.ppermute(sent, GRID, below_pairs)
        turn = layer_index == step
        share = reduced(turn, down_tiles(added(whole_block(pieces), source_narrow)), ROW)
        sent = jnp.where(turn, share, sent)

    both = jnp.stack([share, added(above, source_share)])
    both = copied(both, "z", (zs, *both.shape))
    both = lax.all_gather(both, "core")
    both = both.reshape(cores, cols // 2, 2, 2, group, part).transpose(3, 1, 4, 0, 2, 5)
    both = both.reshape(2, traces, col_width)
    contract = (((1,), (1,)), ((), ()))
    bounced = lax.dot_general(both[1], near_tile, contract, preferred_element_type=F32)


    def times_trans(rows):
        return lax.dot_general(rows, trans_tile, contract, preferred_element_type=F32)

    def share_of_up(turn, passed, cut, shape):
        return lax.cond(
            turn,
            lambda p, b: summed_on_arrival(cut((p + b).astype(BF16)), "col"),
            lambda p, b: jnp.zeros(shape, BF16),
            passed,
            bounced,
        )

    def in_groups(partial):
        tiles = partial.reshape(cols // 2, group, 2, part).transpose(0, 2, 1, 3)
        return tiles.reshape(cols, group, part)

    def in_rows(partial):
        return partial.reshape(cols, few, row_width)

    passed = times_trans(both[0])
    kept = newest = share_of_up(layer_index == layers - 1, passed, in_groups, (group, part))
    for step in range(1, layers):
        pieces = spread(newest, up_pairs, "z")
        if step == layers - 1:
            pair = lax.all_gather(kept, "col", axis_index_groups=neighbours)
            pair = lax.dynamic_slice_in_dim(pair, col_index % 2 * few, few, 1)
            result = pair.transpose(1, 0, 2).reshape(few, row_width)
            pieces, result = lax.optimization_barrier((pieces, result))
        wide = lax.all_gather(pieces, "core").transpose(2, 3, 0, 1, 4)
        passed = times_trans(wide.reshape(traces, col_width))
        turn = layer_index == layers - 1 - step
        if step < layers - 1:
            newest = share_of_up(turn, passed, in_groups, (group, part))
            kept = jnp.where(turn, newest, kept)
        else:
            last = share_of_up(turn, passed, in_rows, (few, row_width))
            result = jnp.where(turn, last, result)
    return result[None]


def solution(mesh):
    layers, rows, cols = mesh.devices.shape
    grid = Mesh(np.array(mesh.devices).reshape(layers, rows // 2, 2, cols), GRID)
    return jax.shard_map(
        per_device,
        mesh=grid,
        in_specs=(P("layer", "col", ROW), P("layer", ROW, "col"), P("layer", ROW, "col")),
        out_specs=P("layer", "col", ROW),
        check_vma=False,
    )
```

```python
import jax
import jax.numpy as jnp
import numpy as np
from jax import lax
from jax.sharding import Mesh, PartitionSpec as P

BF16 = jnp.bfloat16
F32 = jnp.float32
GRID = ("layer", "z", "core", "col")
ROW = ("z", "core")


def copy_for_each(array, axis):
    length = lax.axis_size(axis)
    return lax.all_to_all(
        jnp.broadcast_to(array[None], (length, *array.shape)), axis, 0, 0, tiled=True
    )


def summed_on_arrival(tiles, axis):
    arrived = lax.all_to_all(tiles, axis, split_axis=0, concat_axis=0, tiled=True)
    return arrived.astype(F32).sum(axis=0).astype(BF16)


def added(a, b):
    return (a.astype(F32) + b.astype(F32)).astype(BF16)


def per_device(sources, transmission, reflection):
    layers = lax.axis_size("layer")
    zs = lax.axis_size("z")
    cores = lax.axis_size("core")
    cols = lax.axis_size("col")
    half = zs // 2
    layer_index = lax.axis_index("layer")
    col_index = lax.axis_index("col")
    trans_tile = transmission[0]
    reflect_tile = reflection[0]
    row_width, col_width = trans_tile.shape
    few = sources.shape[1]
    traces = few * cols
    group, part = 2 * few, row_width // 2

    def flat(l, z, k, y):
        return ((l * zs + z) * cores + k) * cols + y

    def cells(layer_range):
        for l in layer_range:
            for z in range(zs):
                for k in range(cores):
                    for y in range(cols):
                        yield l, z, k, y

    far_first = [half, half // 2, zs - half // 2, 0]
    pair_first = [half // 2, half // 4, half - half // 4, 0]
    neighbours = [[i, i + 1] for i in range(0, cols, 2)]

    def down_pairs(d):
        return [
            (flat(l, z, k, y), flat(l + 1, y, z % 2, 2 * ((z // 2 + half // 2 + d) % half) + k))
            for l, z, k, y in cells(range(layers - 1))
        ]

    def up_pairs(d):
        return [
            (flat(l, z, k, y), flat(l - 1, (y + half + d) % zs, k, z))
            for l, z, k, y in cells(range(1, layers))
        ]

    back_pairs = [
        (flat(l, y, k, z), flat(l, z, k, y)) for l, z, k, y in cells(range(layers))
    ]
    below_pairs = [
        (flat(l, z, k, y), flat(l + 1, z, k, y)) for l, z, k, y in cells(range(layers - 1))
    ]

    def spread(share, pairs, axis):
        arrived = [(d, lax.ppermute(share, GRID, pairs(d))) for d in far_first]
        pieces = jnp.zeros((half, *share.shape), BF16)
        for d, piece in arrived:
            place = (lax.axis_index(axis) - half - d) % zs // 2
            pieces = lax.dynamic_update_index_in_dim(pieces, piece, place, 0)
        return lax.all_gather(pieces, axis, axis_index_groups=neighbours)

    def spread_down(share):
        halves = lax.all_gather(share, "core")
        arrived = [(d, lax.ppermute(halves, GRID, down_pairs(d))) for d in pair_first]
        pieces = jnp.zeros((half, *halves.shape), BF16)
        for d, piece in arrived:
            place = (col_index // 2 - half // 2 - d) % half
            pieces = lax.dynamic_update_index_in_dim(pieces, piece, place, 0)
        own_half = lax.dynamic_index_in_dim(halves, lax.axis_index("core"), keepdims=False)
        return pieces, own_half

    def whole_block(pieces):
        halves = lax.all_gather(pieces, "core")
        own_half = lax.dynamic_index_in_dim(halves, lax.axis_index("core"), 2, keepdims=False)
        return own_half.transpose(1, 2, 0, 3).reshape(traces, row_width)

    def down_tiles(incident):
        partial = jnp.dot(incident, trans_tile, preferred_element_type=F32).astype(BF16)
        tiles = partial.reshape(cols // 2, group, cores, 2, part).transpose(0, 3, 2, 1, 4)
        return tiles.reshape(zs * cores, group, part)

    def reduced(turn, tiles, axis):
        return lax.cond(
            turn,
            lambda t: summed_on_arrival(t, axis),
            lambda t: jnp.zeros(t.shape[1:], BF16),
            tiles,
        )

    always = layer_index < layers

    def copied(array, axis, shape):
        return lax.cond(
            always,
            lambda a: copy_for_each(a, axis).reshape(shape),
            lambda a: jnp.zeros(shape, BF16),
            array,
        )

    source_narrow = copied(sources[0], "col", (traces, row_width))
    source_narrow = lax.optimization_barrier(source_narrow)
    own = source_narrow.reshape(cols // 2, group, 2, part).transpose(0, 2, 1, 3)
    own = lax.dynamic_index_in_dim(own.reshape(cols, group, part), col_index, 0, keepdims=False)
    share = reduced(layer_index == 0, down_tiles(source_narrow), ROW)
    sent = share
    for step in range(1, layers):
        pieces, own_half = spread_down(share)
        sent = jnp.where(layer_index == step - 1, own_half, sent)
        if step == 1:
            source_share = lax.ppermute(own, GRID, back_pairs)
            near_tile = jnp.where(always, reflect_tile, jnp.zeros((), BF16))
            pieces, source_share, near_tile = lax.optimization_barrier(
                (pieces, source_share, near_tile)
            )
        if step == layers - 1:
            above = lax.ppermute(sent, GRID, below_pairs)
        turn = layer_index == step
        share = reduced(turn, down_tiles(added(whole_block(pieces), source_narrow)), ROW)

    share, above = lax.optimization_barrier((share, above))
    both = jnp.stack([share, added(above, source_share)])
    both = copied(both, "z", (zs, *both.shape))
    both = lax.all_gather(both, "core")
    both = both.reshape(cores, cols // 2, 2, 2, group, part).transpose(3, 1, 4, 0, 2, 5)
    both = both.reshape(2, traces, col_width)
    contract = (((1,), (1,)), ((), ()))
    bounced = lax.dot_general(both[1], near_tile, contract, preferred_element_type=F32)


    def times_trans(rows):
        return lax.dot_general(rows, trans_tile, contract, preferred_element_type=F32)

    def share_of_up(turn, passed, cut, shape):
        return lax.cond(
            turn,
            lambda p, b: summed_on_arrival(cut((p + b).astype(BF16)), "col"),
            lambda p, b: jnp.zeros(shape, BF16),
            passed,
            bounced,
        )

    def in_groups(partial):
        tiles = partial.reshape(cols // 2, group, 2, part).transpose(0, 2, 1, 3)
        return tiles.reshape(cols, group, part)

    def in_rows(partial):
        return partial.reshape(cols, few, row_width)

    passed = times_trans(both[0])
    kept = newest = share_of_up(layer_index == layers - 1, passed, in_groups, (group, part))
    for step in range(1, layers):
        pieces = spread(newest, up_pairs, "z")
        if step == layers - 1:
            pair = lax.all_gather(kept, "col", axis_index_groups=neighbours)
            pair = lax.dynamic_slice_in_dim(pair, col_index % 2 * few, few, 1)
            result = pair.transpose(1, 0, 2).reshape(few, row_width)
            pieces, result = lax.optimization_barrier((pieces, result))
        wide = lax.all_gather(pieces, "core").transpose(2, 3, 0, 1, 4)
        passed = times_trans(wide.reshape(traces, col_width))
        turn = layer_index == layers - 1 - step
        if step < layers - 1:
            newest = share_of_up(turn, passed, in_groups, (group, part))
            kept = jnp.where(turn, newest, kept)
        else:
            last = share_of_up(turn, passed, in_rows, (few, row_width))
            result = jnp.where(turn, last, result)
    return result[None]


def solution(mesh):
    layers, rows, cols = mesh.devices.shape
    grid = Mesh(np.array(mesh.devices).reshape(layers, rows // 2, 2, cols), GRID)
    return jax.shard_map(
        per_device,
        mesh=grid,
        in_specs=(P("layer", "col", ROW), P("layer", ROW, "col"), P("layer", ROW, "col")),
        out_specs=P("layer", "col", ROW),
        check_vma=False,
    )
```

```python
import jax
import jax.numpy as jnp
import numpy as np
from jax import lax
from jax.sharding import Mesh, PartitionSpec as P

BF16 = jnp.bfloat16
F32 = jnp.float32
GRID = ("layer", "z", "core", "col")
ROW = ("z", "core")


def copy_for_each(array, axis):
    length = lax.axis_size(axis)
    return lax.all_to_all(
        jnp.broadcast_to(array[None], (length, *array.shape)), axis, 0, 0, tiled=True
    )


def summed_on_arrival(tiles, axis):
    arrived = lax.all_to_all(tiles, axis, split_axis=0, concat_axis=0, tiled=True)
    return arrived.astype(F32).sum(axis=0).astype(BF16)


def added(a, b):
    return (a.astype(F32) + b.astype(F32)).astype(BF16)


def per_device(sources, transmission, reflection):
    layers = lax.axis_size("layer")
    zs = lax.axis_size("z")
    cores = lax.axis_size("core")
    cols = lax.axis_size("col")
    half = zs // 2
    layer_index = lax.axis_index("layer")
    col_index = lax.axis_index("col")
    trans_tile = transmission[0]
    reflect_tile = reflection[0]
    row_width, col_width = trans_tile.shape
    few = sources.shape[1]
    traces = few * cols
    group, part = 2 * few, row_width // 2

    def flat(l, z, k, y):
        return ((l * zs + z) * cores + k) * cols + y

    def cells(layer_range):
        for l in layer_range:
            for z in range(zs):
                for k in range(cores):
                    for y in range(cols):
                        yield l, z, k, y

    far_first = [half, half // 2, zs - half // 2, 0]
    neighbours = [[i, i + 1] for i in range(0, cols, 2)]

    def down_pairs(d):
        return [
            (flat(l, z, k, y), flat(l + 1, y, k, (z + half + d) % zs))
            for l, z, k, y in cells(range(layers - 1))
        ]

    def up_pairs(d):
        return [
            (flat(l, z, k, y), flat(l - 1, (y + half + d) % zs, k, z))
            for l, z, k, y in cells(range(1, layers))
        ]

    back_pairs = [
        (flat(l, y, k, z), flat(l, z, k, y)) for l, z, k, y in cells(range(layers))
    ]
    below_pairs = [
        (flat(l, z, k, y), flat(l + 1, z, k, y)) for l, z, k, y in cells(range(layers - 1))
    ]

    def spread(share, pairs, axis):
        arrived = [(d, lax.ppermute(share, GRID, pairs(d))) for d in far_first]
        pieces = jnp.zeros((half, *share.shape), BF16)
        for d, piece in arrived:
            place = (lax.axis_index(axis) - half - d) % zs // 2
            pieces = lax.dynamic_update_index_in_dim(pieces, piece, place, 0)
        return lax.all_gather(pieces, axis, axis_index_groups=neighbours)

    def whole_block(pieces):
        return pieces.transpose(1, 2, 0, 3).reshape(traces, row_width)

    def down_tiles(incident):
        partial = jnp.dot(incident, trans_tile, preferred_element_type=F32).astype(BF16)
        tiles = partial.reshape(cols // 2, group, cores, 2, part).transpose(0, 3, 2, 1, 4)
        return tiles.reshape(zs * cores, group, part)

    def reduced(turn, tiles, axis):
        return lax.cond(
            turn,
            lambda t: summed_on_arrival(t, axis),
            lambda t: jnp.zeros(t.shape[1:], BF16),
            tiles,
        )

    always = layer_index < layers

    def copied(array, axis, shape):
        return lax.cond(
            always,
            lambda a: copy_for_each(a, axis).reshape(shape),
            lambda a: jnp.zeros(shape, BF16),
            array,
        )

    source_narrow = copied(sources[0], "col", (traces, row_width))
    source_narrow = lax.optimization_barrier(source_narrow)
    own = source_narrow.reshape(cols // 2, group, 2, part).transpose(0, 2, 1, 3)
    own = lax.dynamic_index_in_dim(own.reshape(cols, group, part), col_index, 0, keepdims=False)
    share = reduced(layer_index == 0, down_tiles(source_narrow), ROW)
    sent = share
    for step in range(1, layers):
        pieces = spread(share, down_pairs, "col")
        if step == 1:
            source_share = lax.ppermute(own, GRID, back_pairs)
            near_tile = jnp.where(always, reflect_tile, jnp.zeros((), BF16))
            pieces, source_share, near_tile = lax.optimization_barrier(
                (pieces, source_share, near_tile)
            )
        if step == layers - 1:
            above = lax.ppermute(sent, GRID, below_pairs)
        turn = layer_index == step
        share = reduced(turn, down_tiles(added(whole_block(pieces), source_narrow)), ROW)
        sent = jnp.where(turn, share, sent)

    both = jnp.stack([share, added(above, source_share)])
    both = copied(both, "z", (zs, *both.shape))
    both = lax.all_gather(both, "core")
    both = both.reshape(cores, cols // 2, 2, 2, group, part).transpose(3, 1, 4, 0, 2, 5)
    both = both.reshape(2, traces, col_width)
    contract = (((1,), (1,)), ((), ()))
    bounced = lax.dot_general(both[1], near_tile, contract, preferred_element_type=F32)


    def times_trans(rows):
        return lax.dot_general(rows, trans_tile, contract, preferred_element_type=F32)

    def share_of_up(turn, passed, cut, shape):
        return lax.cond(
            turn,
            lambda p, b: summed_on_arrival(cut((p + b).astype(BF16)), "col"),
            lambda p, b: jnp.zeros(shape, BF16),
            passed,
            bounced,
        )

    def in_groups(partial):
        tiles = partial.reshape(cols // 2, group, 2, part).transpose(0, 2, 1, 3)
        return tiles.reshape(cols, group, part)

    tail = few - 8

    def packed(partial):
        rows = partial.reshape(cols, few, row_width)
        rest = rows[:, 8:].reshape(cols, tail, 2, part).transpose(0, 2, 1, 3)
        return jnp.concatenate([rows[:, :8], rest.reshape(cols, 8, part)], axis=2)

    def unpacked(rows):
        rest = rows[:, row_width:].reshape(2, tail, part).transpose(1, 0, 2)
        return jnp.concatenate([rows[:, :row_width], rest.reshape(tail, row_width)])

    passed = times_trans(both[0])
    kept = newest = share_of_up(layer_index == layers - 1, passed, in_groups, (group, part))
    for step in range(1, layers):
        pieces = spread(newest, up_pairs, "z")
        if step == layers - 1:
            pair = lax.all_gather(kept, "col", axis_index_groups=neighbours)
            pair = lax.dynamic_slice_in_dim(pair, col_index % 2 * few, few, 1)
            result = pair.transpose(1, 0, 2).reshape(few, row_width)
            pieces, result = lax.optimization_barrier((pieces, result))
        wide = lax.all_gather(pieces, "core").transpose(2, 3, 0, 1, 4)
        passed = times_trans(wide.reshape(traces, col_width))
        turn = layer_index == layers - 1 - step
        if step < layers - 1:
            newest = share_of_up(turn, passed, in_groups, (group, part))
            kept = jnp.where(turn, newest, kept)
        else:
            last = share_of_up(turn, passed, packed, (8, row_width + part))
            result = jnp.where(turn, unpacked(last), result)
    return result[None]


def solution(mesh):
    layers, rows, cols = mesh.devices.shape
    grid = Mesh(np.array(mesh.devices).reshape(layers, rows // 2, 2, cols), GRID)
    return jax.shard_map(
        per_device,
        mesh=grid,
        in_specs=(P("layer", "col", ROW), P("layer", ROW, "col"), P("layer", ROW, "col")),
        out_specs=P("layer", "col", ROW),
        check_vma=False,
    )
```

```python
import jax
import jax.numpy as jnp
import numpy as np
from jax import lax
from jax.sharding import Mesh, PartitionSpec as P

BF16 = jnp.bfloat16
F32 = jnp.float32
GRID = ("layer", "z", "core", "col")
ROW = ("z", "core")


def copy_for_each(array, axis):
    length = lax.axis_size(axis)
    return lax.all_to_all(
        jnp.broadcast_to(array[None], (length, *array.shape)), axis, 0, 0, tiled=True
    )


def summed_on_arrival(tiles, axis):
    arrived = lax.all_to_all(tiles, axis, split_axis=0, concat_axis=0, tiled=True)
    return arrived.astype(F32).sum(axis=0).astype(BF16)


def added(a, b):
    return (a.astype(F32) + b.astype(F32)).astype(BF16)


def per_device(sources, transmission, reflection):
    layers = lax.axis_size("layer")
    zs = lax.axis_size("z")
    cores = lax.axis_size("core")
    cols = lax.axis_size("col")
    half = zs // 2
    layer_index = lax.axis_index("layer")
    col_index = lax.axis_index("col")
    trans_tile = transmission[0]
    reflect_tile = reflection[0]
    row_width, col_width = trans_tile.shape
    few = sources.shape[1]
    traces = few * cols
    group, part = 2 * few, row_width // 2

    def flat(l, z, k, y):
        return ((l * zs + z) * cores + k) * cols + y

    def cells(layer_range):
        for l in layer_range:
            for z in range(zs):
                for k in range(cores):
                    for y in range(cols):
                        yield l, z, k, y

    far_first = [half, half // 2, zs - half // 2, 0]
    neighbours = [[i, i + 1] for i in range(0, cols, 2)]

    def down_pairs(d):
        return [
            (flat(l, z, k, y), flat(l + 1, y, k, (z + half + d) % zs))
            for l, z, k, y in cells(range(layers - 1))
        ]

    def up_pairs(d):
        return [
            (flat(l, z, k, y), flat(l - 1, (y + half + d) % zs, k, z))
            for l, z, k, y in cells(range(1, layers))
        ]

    back_pairs = [
        (flat(l, y, k, z), flat(l, z, k, y)) for l, z, k, y in cells(range(layers))
    ]
    below_pairs = [
        (flat(l, z, k, y), flat(l + 1, z, k, y)) for l, z, k, y in cells(range(layers - 1))
    ]

    def spread(share, pairs, axis):
        arrived = [lax.ppermute(share, GRID, pairs(d)) for d in far_first]
        pieces = jnp.zeros((2, half, *share.shape), BF16)
        exchanged = []
        for start in (0, 2):
            two = arrived[start : start + 2]
            if exchanged:
                two[0], two[1], exchanged[0] = lax.optimization_barrier((*two, exchanged[0]))
            both_parities = lax.all_gather(jnp.stack(two), axis, axis_index_groups=neighbours)
            exchanged.append(both_parities)
        for number, d in enumerate(far_first):
            place = (lax.axis_index(axis) - half - d) % zs // 2
            piece = exchanged[number // 2][:, number % 2]
            pieces = lax.dynamic_update_index_in_dim(pieces, piece, place, 1)
        return pieces

    def whole_block(pieces):
        return pieces.transpose(1, 2, 0, 3).reshape(traces, row_width)

    def down_tiles(incident):
        partial = jnp.dot(incident, trans_tile, preferred_element_type=F32).astype(BF16)
        tiles = partial.reshape(cols // 2, group, cores, 2, part).transpose(0, 3, 2, 1, 4)
        return tiles.reshape(zs * cores, group, part)

    def reduced(turn, tiles, axis):
        return lax.cond(
            turn,
            lambda t: summed_on_arrival(t, axis),
            lambda t: jnp.zeros(t.shape[1:], BF16),
            tiles,
        )

    always = layer_index < layers

    def copied(array, axis, shape):
        return lax.cond(
            always,
            lambda a: copy_for_each(a, axis).reshape(shape),
            lambda a: jnp.zeros(shape, BF16),
            array,
        )

    source_narrow = copied(sources[0], "col", (traces, row_width))
    source_narrow = lax.optimization_barrier(source_narrow)
    own = source_narrow.reshape(cols // 2, group, 2, part).transpose(0, 2, 1, 3)
    own = lax.dynamic_index_in_dim(own.reshape(cols, group, part), col_index, 0, keepdims=False)
    share = reduced(layer_index == 0, down_tiles(source_narrow), ROW)
    sent = share
    for step in range(1, layers):
        pieces = spread(share, down_pairs, "col")
        if step == 1:
            source_share = lax.ppermute(own, GRID, back_pairs)
            near_tile = jnp.where(always, reflect_tile, jnp.zeros((), BF16))
            pieces, source_share, near_tile = lax.optimization_barrier(
                (pieces, source_share, near_tile)
            )
        if step == layers - 1:
            above = lax.ppermute(sent, GRID, below_pairs)
        turn = layer_index == step
        share = reduced(turn, down_tiles(added(whole_block(pieces), source_narrow)), ROW)
        sent = jnp.where(turn, share, sent)

    both = jnp.stack([share, added(above, source_share)])
    both = copied(both, "z", (zs, *both.shape))
    both = lax.all_gather(both, "core")
    both = both.reshape(cores, cols // 2, 2, 2, group, part).transpose(3, 1, 4, 0, 2, 5)
    both = both.reshape(2, traces, col_width)
    contract = (((1,), (1,)), ((), ()))
    bounced = lax.dot_general(both[1], near_tile, contract, preferred_element_type=F32)


    def times_trans(rows):
        return lax.dot_general(rows, trans_tile, contract, preferred_element_type=F32)

    def share_of_up(turn, passed, cut, shape):
        return lax.cond(
            turn,
            lambda p, b: summed_on_arrival(cut((p + b).astype(BF16)), "col"),
            lambda p, b: jnp.zeros(shape, BF16),
            passed,
            bounced,
        )

    def in_groups(partial):
        tiles = partial.reshape(cols // 2, group, 2, part).transpose(0, 2, 1, 3)
        return tiles.reshape(cols, group, part)

    tail = few - 8

    def packed(partial):
        rows = partial.reshape(cols, few, row_width)
        rest = rows[:, 8:].reshape(cols, tail, 2, part).transpose(0, 2, 1, 3)
        return jnp.concatenate([rows[:, :8], rest.reshape(cols, 8, part)], axis=2)

    def unpacked(rows):
        rest = rows[:, row_width:].reshape(2, tail, part).transpose(1, 0, 2)
        return jnp.concatenate([rows[:, :row_width], rest.reshape(tail, row_width)])

    passed = times_trans(both[0])
    kept = newest = share_of_up(layer_index == layers - 1, passed, in_groups, (group, part))
    for step in range(1, layers):
        pieces = spread(newest, up_pairs, "z")
        if step == layers - 1:
            pair = lax.all_gather(kept, "col", axis_index_groups=neighbours)
            pair = lax.dynamic_slice_in_dim(pair, col_index % 2 * few, few, 1)
            result = pair.transpose(1, 0, 2).reshape(few, row_width)
            pieces, result = lax.optimization_barrier((pieces, result))
        wide = lax.all_gather(pieces, "core").transpose(2, 3, 0, 1, 4)
        passed = times_trans(wide.reshape(traces, col_width))
        turn = layer_index == layers - 1 - step
        if step < layers - 1:
            newest = share_of_up(turn, passed, in_groups, (group, part))
            kept = jnp.where(turn, newest, kept)
        else:
            last = share_of_up(turn, passed, packed, (8, row_width + part))
            result = jnp.where(turn, unpacked(last), result)
    return result[None]


def solution(mesh):
    layers, rows, cols = mesh.devices.shape
    grid = Mesh(np.array(mesh.devices).reshape(layers, rows // 2, 2, cols), GRID)
    return jax.shard_map(
        per_device,
        mesh=grid,
        in_specs=(P("layer", "col", ROW), P("layer", ROW, "col"), P("layer", ROW, "col")),
        out_specs=P("layer", "col", ROW),
        check_vma=False,
    )
```

```python
import jax
import jax.numpy as jnp
import numpy as np
from jax import lax
from jax.sharding import Mesh, PartitionSpec as P

BF16 = jnp.bfloat16
F32 = jnp.float32
GRID = ("layer", "z", "core", "col")
ROW = ("z", "core")


def copy_for_each(array, axis):
    length = lax.axis_size(axis)
    return lax.all_to_all(
        jnp.broadcast_to(array[None], (length, *array.shape)), axis, 0, 0, tiled=True
    )


def summed_on_arrival(tiles, axis):
    arrived = lax.all_to_all(tiles, axis, split_axis=0, concat_axis=0, tiled=True)
    return arrived.astype(F32).sum(axis=0).astype(BF16)


def added(a, b):
    return (a.astype(F32) + b.astype(F32)).astype(BF16)


def per_device(sources, transmission, reflection):
    layers = lax.axis_size("layer")
    zs = lax.axis_size("z")
    cores = lax.axis_size("core")
    cols = lax.axis_size("col")
    half = zs // 2
    layer_index = lax.axis_index("layer")
    col_index = lax.axis_index("col")
    trans_tile = transmission[0]
    reflect_tile = reflection[0]
    row_width, col_width = trans_tile.shape
    few = sources.shape[1]
    traces = few * cols
    group, part = 2 * few, row_width // 2

    def flat(l, z, k, y):
        return ((l * zs + z) * cores + k) * cols + y

    def cells(layer_range):
        for l in layer_range:
            for z in range(zs):
                for k in range(cores):
                    for y in range(cols):
                        yield l, z, k, y

    near_first = [0, half // 2, zs - half // 2, half]
    neighbours = [[i, i + 1] for i in range(0, cols, 2)]

    def down_pairs(d):
        return [
            (flat(l, z, k, y), flat(l + 1, y, k, (z + half + d) % zs))
            for l, z, k, y in cells(range(layers - 1))
        ]

    def up_pairs(d):
        return [
            (flat(l, z, k, y), flat(l - 1, (y + half + d) % zs, k, z))
            for l, z, k, y in cells(range(1, layers))
        ]

    back_pairs = [
        (flat(l, y, k, z), flat(l, z, k, y)) for l, z, k, y in cells(range(layers))
    ]
    below_pairs = [
        (flat(l, z, k, y), flat(l + 1, z, k, y)) for l, z, k, y in cells(range(layers - 1))
    ]

    def spread(share, pairs, axis):
        arrived = [(d, lax.ppermute(share, GRID, pairs(d))) for d in near_first]
        pieces = jnp.zeros((half, *share.shape), BF16)
        for d, piece in arrived:
            place = (lax.axis_index(axis) - half - d) % zs // 2
            pieces = lax.dynamic_update_index_in_dim(pieces, piece, place, 0)
        return lax.all_gather(pieces, axis, axis_index_groups=neighbours)

    def whole_block(pieces):
        return pieces.transpose(1, 2, 0, 3).reshape(traces, row_width)

    def down_tiles(incident):
        partial = jnp.dot(incident, trans_tile, preferred_element_type=F32).astype(BF16)
        tiles = partial.reshape(cols // 2, group, cores, 2, part).transpose(0, 3, 2, 1, 4)
        return tiles.reshape(zs * cores, group, part)

    def reduced(turn, tiles, axis):
        return lax.cond(
            turn,
            lambda t: summed_on_arrival(t, axis),
            lambda t: jnp.zeros(t.shape[1:], BF16),
            tiles,
        )

    always = layer_index < layers

    def copied(array, axis, shape):
        return lax.cond(
            always,
            lambda a: copy_for_each(a, axis).reshape(shape),
            lambda a: jnp.zeros(shape, BF16),
            array,
        )

    source_narrow = copied(sources[0], "col", (traces, row_width))
    source_narrow = lax.optimization_barrier(source_narrow)
    own = source_narrow.reshape(cols // 2, group, 2, part).transpose(0, 2, 1, 3)
    own = lax.dynamic_index_in_dim(own.reshape(cols, group, part), col_index, 0, keepdims=False)
    share = reduced(layer_index == 0, down_tiles(source_narrow), ROW)
    sent = share
    for step in range(1, layers):
        pieces = spread(share, down_pairs, "col")
        if step == 1:
            source_share = lax.ppermute(own, GRID, back_pairs)
            near_tile = jnp.where(always, reflect_tile, jnp.zeros((), BF16))
            pieces, source_share, near_tile = lax.optimization_barrier(
                (pieces, source_share, near_tile)
            )
        if step == layers - 1:
            above = lax.ppermute(sent, GRID, below_pairs)
        turn = layer_index == step
        share = reduced(turn, down_tiles(added(whole_block(pieces), source_narrow)), ROW)
        sent = jnp.where(turn, share, sent)

    both = jnp.stack([share, added(above, source_share)])
    both = copied(both, "z", (zs, *both.shape))
    both = lax.all_gather(both, "core")
    both = both.reshape(cores, cols // 2, 2, 2, group, part).transpose(3, 1, 4, 0, 2, 5)
    both = both.reshape(2, traces, col_width)
    contract = (((1,), (1,)), ((), ()))
    bounced = lax.dot_general(both[1], near_tile, contract, preferred_element_type=F32)


    def times_trans(rows):
        return lax.dot_general(rows, trans_tile, contract, preferred_element_type=F32)

    def share_of_up(turn, passed, cut, shape):
        return lax.cond(
            turn,
            lambda p, b: summed_on_arrival(cut((p + b).astype(BF16)), "col"),
            lambda p, b: jnp.zeros(shape, BF16),
            passed,
            bounced,
        )

    def in_groups(partial):
        tiles = partial.reshape(cols // 2, group, 2, part).transpose(0, 2, 1, 3)
        return tiles.reshape(cols, group, part)

    tail = few - 8

    def packed(partial):
        rows = partial.reshape(cols, few, row_width)
        rest = rows[:, 8:].reshape(cols, tail, 2, part).transpose(0, 2, 1, 3)
        return jnp.concatenate([rows[:, :8], rest.reshape(cols, 8, part)], axis=2)

    def unpacked(rows):
        rest = rows[:, row_width:].reshape(2, tail, part).transpose(1, 0, 2)
        return jnp.concatenate([rows[:, :row_width], rest.reshape(tail, row_width)])

    passed = times_trans(both[0])
    kept = newest = share_of_up(layer_index == layers - 1, passed, in_groups, (group, part))
    for step in range(1, layers):
        pieces = spread(newest, up_pairs, "z")
        if step == layers - 1:
            pair = lax.all_gather(kept, "col", axis_index_groups=neighbours)
            pair = lax.dynamic_slice_in_dim(pair, col_index % 2 * few, few, 1)
            result = pair.transpose(1, 0, 2).reshape(few, row_width)
            pieces, result = lax.optimization_barrier((pieces, result))
        wide = lax.all_gather(pieces, "core").transpose(2, 3, 0, 1, 4)
        passed = times_trans(wide.reshape(traces, col_width))
        turn = layer_index == layers - 1 - step
        if step < layers - 1:
            newest = share_of_up(turn, passed, in_groups, (group, part))
            kept = jnp.where(turn, newest, kept)
        else:
            last = share_of_up(turn, passed, packed, (8, row_width + part))
            result = jnp.where(turn, unpacked(last), result)
    return result[None]


def solution(mesh):
    layers, rows, cols = mesh.devices.shape
    grid = Mesh(np.array(mesh.devices).reshape(layers, rows // 2, 2, cols), GRID)
    return jax.shard_map(
        per_device,
        mesh=grid,
        in_specs=(P("layer", "col", ROW), P("layer", ROW, "col"), P("layer", ROW, "col")),
        out_specs=P("layer", "col", ROW),
        check_vma=False,
    )
```
